32 devices in a mesh: dp: 8 (over y, x, core), mp: 4 (over z).
Axes of the slice: x: 2, y: 2, z: 4, core: 2. Of those that a mesh axis runs over, the one named last changes fastest.
Arguments:
- grad_parts: bfloat16 [8, 1, 6144, 6144], P('dp', None, None, 'mp'), may hold values from -6 to 6
- master: float32 [1, 6144, 6144], P(None, 'dp', 'mp'), may hold values from -6 to 6
- momentum: float32 [1, 6144, 6144], P(None, 'dp', 'mp'), may hold values from -4 to 4
Outputs:
- new_master: float32 [1, 6144, 6144], P(None, 'dp', 'mp')
- new_momentum: float32 [1, 6144, 6144], P(None, 'dp', 'mp')
- new_weights: bfloat16 [1, 6144, 6144], P(None, None, 'mp')
The draws below stay inside these ranges and needn't reach their ends.
All inputs are finite; a program needn't handle non-finite values.
Results may differ from the reference program's by a relative error of at most 0.0014.
Values may be sent and summed in bfloat16 or wider, within the bound.
A program may use at most 128 MiB of HBM per device.

```python
import jax
import jax.numpy as jnp
from jax import lax

D = 6144
LAYERS = 1
INNER = 6144
REPLICAS = 8


def spiked(drawn, rng, source, target, blocks, factor):
    owner, partner = [(jnp.arange(drawn.shape[axis_at]) // (drawn.shape[axis_at] // blocks)).reshape([-1 if axis == axis_at else 1 for axis in range(drawn.ndim)]) for axis_at in (source, target)]
    chosen = jax.random.permutation(rng, blocks)[partner]
    strong = (owner == chosen) | (owner == (partner + blocks // 2) % blocks)
    return jnp.where(strong, factor * drawn, drawn)


def levels(rng, dims, split, smallest, largest):
    factor_of = 1.0
    for axis_at, blocks in split:
        draws = jax.random.uniform(jax.random.fold_in(jax.random.fold_in(rng, 6), axis_at), (blocks,), jnp.float32, smallest / len(split), largest / len(split))
        factor_of = factor_of * jnp.repeat(jnp.exp(draws), dims[axis_at] // blocks).reshape((-1,) + (1,) * (len(dims) - 1 - axis_at))
    return factor_of


def bell_draw(own_key, extent, deviation, bound, cuts=(), held_as=jnp.bfloat16):
    values = deviation * jax.random.normal(own_key, extent, jnp.float32)
    if cuts:
        values = values * levels(own_key, extent, cuts, -0.22, 0.18)
    return jnp.clip(values, -bound, bound).astype(held_as)


def gaussian_with(stream_key, dims, spread, reach, shards, heavy, held_as=jnp.bfloat16):
    drawn = spread * jax.random.normal(stream_key, dims, jnp.float32)
    if shards:
        drawn = drawn * levels(stream_key, dims, shards, -0.22, 0.18)
    return jnp.clip(spiked(drawn, jax.random.fold_in(stream_key, 3), *heavy), -reach, reach).astype(held_as)


def setup_inputs(seed: int = 0) -> dict:
    seeds = jax.random.split(jax.random.key(seed), 4)
    grad_parts = gaussian_with(seeds[0], (REPLICAS, LAYERS, INNER, D), 1.0, 6.0, ((0, 8), (3, 4)), (0, 2, 8, 2.0))
    master = bell_draw(seeds[1], (LAYERS, INNER, D), 1.0, 6.0, ((1, 8), (2, 4)), jnp.float32)
    momentum = bell_draw(seeds[2], (LAYERS, INNER, D), 0.25, 4.0, ((1, 8), (2, 4)), jnp.float32)
    return dict(grad_parts=grad_parts, master=master, momentum=momentum)


beta_one = 0.9
beta_two = 0.99
step_size = 0.1
decay_rate = 0.1
softness = 0.05

def reference(grad_parts, master, momentum):
    gradient = lax.optimization_barrier(jnp.sum(grad_parts.astype(jnp.float32), axis=0)) / REPLICAS
    interp = beta_one * momentum + (1.0 - beta_one) * gradient
    direction = interp / jnp.sqrt(interp * interp + softness * softness)
    new_master = master - step_size * (direction + decay_rate * master)
    new_momentum = beta_two * momentum + (1.0 - beta_two) * gradient
    return (new_master, new_momentum, new_master.astype(jnp.bfloat16))
```

```python
import functools

import jax
import jax.numpy as jnp
from jax import lax
from jax.experimental import pallas as pl
from jax.experimental.pallas import tpu as pltpu
from jax.sharding import PartitionSpec as P

beta_one = 0.9
beta_two = 0.99
step_size = 0.1
decay_rate = 0.1
softness = 0.05

f32 = jnp.float32
bf16 = jnp.bfloat16
MESH = pl.DeviceIdType.MESH
ROWS = 16
MOST_CHUNKS = 8


def factors(n):
    cores = 2
    across = 2
    return n // (cores * across), across, cores


def kernel(
    dims,
    g_ref, master_ref, momentum_ref,
    nmaster, nmomentum, w,
    own, pair, p1, q1, p2, q2,
    load_sem, state_sem,
    pair_s, pair_r, p1_s, p1_r, q1_s, q1_r, p2_s, p2_r, q2_s, q2_r,
    ay_s, ay_r, ax_s, ax_r, rx_s, rx_r, ry_s, ry_r,
    d0_s, d0_r, dy_s, dy_r, dx_s, dx_r, dp_s, dp_r, dq_s, dq_r,
):
    Y, X, C, K, c = dims
    me = lax.axis_index("dp")
    core = lax.rem(me, C)
    mx = lax.rem(me // C, X)
    my = me // (C * X)
    other = 1 - core

    def index(y, x, k):
        return {"dp": (y * X + x) * C + k}

    mate = index(my, mx, other)

    def plus(a, j, size):
        return lax.rem(a + j, size)

    def minus(a, j, size):
        return lax.rem(a + size - j, size)

    ys, xs = range(1, Y), range(1, X)

    def remote(src, dst, s, r, to):
        return pltpu.make_async_remote_copy(
            src_ref=src, dst_ref=dst, send_sem=s, recv_sem=r,
            device_id=to, device_id_type=MESH,
        )

    def load(k):
        return pltpu.make_async_copy(g_ref.at[:, :, core, :, k], own.at[k], load_sem.at[k])

    def state(k):
        return (
            pltpu.make_async_copy(master_ref.at[:, k], nmaster.at[:, k], state_sem.at[0, k]),
            pltpu.make_async_copy(momentum_ref.at[:, k], nmomentum.at[:, k], state_sem.at[1, k]),
        )

    def pair_copy(k):
        return remote(g_ref.at[:, :, other, :, k], pair.at[k], pair_s.at[k], pair_r.at[k], mate)

    def p1_copy(j, k):
        to = plus(mx, j, X)
        return remote(own.at[k, :, to, 0], p1.at[j - 1, k], p1_s.at[j - 1, k], p1_r.at[j - 1, k], index(my, to, core))

    def q1_copy(j, k):
        to = plus(my, j, Y)
        return remote(own.at[k, to, :, 1], q1.at[j - 1, k], q1_s.at[j - 1, k], q1_r.at[j - 1, k], index(to, mx, core))

    def p2_copy(j, k):
        to = plus(my, j, Y)
        return remote(own.at[k, to, mx, 0], p2.at[j - 1, k], p2_s.at[j - 1, k], p2_r.at[j - 1, k], index(to, mx, core))

    def q2_copy(j, k):
        to = plus(mx, j, X)
        return remote(own.at[k, my, to, 1], q2.at[j - 1, k], q2_s.at[j - 1, k], q2_r.at[j - 1, k], index(my, to, core))

    def spread(block, s, r, to):
        return remote(block, block, s, r, to)

    def ay_copy(j, k, y):
        return spread(w.at[y, mx, core, :, k], ay_s.at[j - 1, k], ay_r.at[j - 1, k], index(plus(my, j, Y), mx, core))

    def ax_copy(j, k, x):
        return spread(w.at[my, x, core, :, k], ax_s.at[j - 1, k], ax_r.at[j - 1, k], index(my, plus(mx, j, X), core))

    def rx_copy(jx, jy, k, x):
        y = minus(my, jy, Y)
        return spread(w.at[y, x, core, 0, k], rx_s.at[jx - 1, jy - 1, k], rx_r.at[jx - 1, jy - 1, k], index(my, plus(mx, jx, X), core))

    def ry_copy(jx, jy, k, y):
        x = minus(mx, jx, X)
        return spread(w.at[y, x, core, 1, k], ry_s.at[jx - 1, jy - 1, k], ry_r.at[jx - 1, jy - 1, k], index(plus(my, jy, Y), mx, core))

    def d0_copy(k, half):
        return spread(w.at[my, mx, half, :, k], d0_s.at[k], d0_r.at[k], mate)

    def dy_copy(j, k, half):
        return spread(w.at[minus(my, j, Y), mx, half, :, k], dy_s.at[j - 1, k], dy_r.at[j - 1, k], mate)

    def dx_copy(j, k, half):
        return spread(w.at[my, minus(mx, j, X), half, :, k], dx_s.at[j - 1, k], dx_r.at[j - 1, k], mate)

    def dp_copy(jx, jy, k, half):
        return spread(w.at[minus(my, jy, Y), minus(mx, jx, X), half, 0, k], dp_s.at[jx - 1, jy - 1, k], dp_r.at[jx - 1, jy - 1, k], mate)

    def dq_copy(jx, jy, k, half):
        return spread(w.at[minus(my, jy, Y), minus(mx, jx, X), half, 1, k], dq_s.at[jx - 1, jy - 1, k], dq_r.at[jx - 1, jy - 1, k], mate)

    def each(body):
        lax.fori_loop(0, K, lambda k, carry: (body(k), carry)[1], 0)

    def rows(body):
        lax.fori_loop(0, c // ROWS, lambda r, carry: (body(pl.ds(pl.multiple_of(r * ROWS, ROWS), ROWS)), carry)[1], 0)

    def start_loads(k):
        load(k).start()

    def start_state(k):
        for copy in state(k):
            copy.start()

    each(start_loads)

    barrier = pltpu.get_barrier_semaphore()
    peers = [mate]
    peers += [index(my, plus(mx, j, X), core) for j in xs]
    peers += [index(plus(my, j, Y), mx, core) for j in ys]
    for peer in peers:
        pl.semaphore_signal(barrier, inc=1, device_id=peer, device_id_type=MESH)
    pl.semaphore_wait(barrier, len(peers))

    each(lambda k: pair_copy(k).start())
    each(start_state)

    def first(k):
        load(k).wait()
        pair_copy(k).wait_recv()

        def add(r):
            for j in xs:
                x = plus(mx, j, X)
                for y in range(Y):
                    own[k, y, x, 0, r] = (own[k, y, x, 0, r].astype(f32) + pair[k, y, x, 0, r].astype(f32)).astype(bf16)
            for j in ys:
                y = plus(my, j, Y)
                for x in range(X):
                    own[k, y, x, 1, r] = (own[k, y, x, 1, r].astype(f32) + pair[k, y, x, 1, r].astype(f32)).astype(bf16)

        rows(add)
        for j in xs:
            p1_copy(j, k).start()
        for j in ys:
            q1_copy(j, k).start()

    each(first)

    def p_sum(k, y, r):
        total = own[k, y, mx, 0, r].astype(f32) + pair[k, y, mx, 0, r].astype(f32)
        for j in xs:
            total += p1[j - 1, k, y, r].astype(f32)
        return total

    def q_sum(k, x, r):
        total = own[k, my, x, 1, r].astype(f32) + pair[k, my, x, 1, r].astype(f32)
        for j in ys:
            total += q1[j - 1, k, x, r].astype(f32)
        return total

    def second(k):
        for j in xs:
            p1_copy(j, k).wait_recv()
        for j in ys:
            q1_copy(j, k).wait_recv()

        def add(r):
            for j in ys:
                y = plus(my, j, Y)
                own[k, y, mx, 0, r] = p_sum(k, y, r).astype(bf16)
            for j in xs:
                x = plus(mx, j, X)
                own[k, my, x, 1, r] = q_sum(k, x, r).astype(bf16)

        rows(add)
        for j in ys:
            p2_copy(j, k).start()
        for j in xs:
            q2_copy(j, k).start()

    each(second)

    def step(total, h, k, r):
        gradient = total * (1.0 / (Y * X * C))
        momentum = nmomentum[h, k, r]
        master = nmaster[h, k, r]
        interp = beta_one * momentum + (1.0 - beta_one) * gradient
        direction = interp * lax.rsqrt(interp * interp + softness * softness)
        new_master = master - step_size * (direction + decay_rate * master)
        nmaster[h, k, r] = new_master
        nmomentum[h, k, r] = beta_two * momentum + (1.0 - beta_two) * gradient
        w[my, mx, core, h, k, r] = new_master.astype(bf16)

    def third(k):
        for copy in state(k):
            copy.wait()
        for j in ys:
            p2_copy(j, k).wait_recv()
        for j in xs:
            q2_copy(j, k).wait_recv()

        def update(r):
            total = p_sum(k, my, r)
            for j in ys:
                total += p2[j - 1, k, r].astype(f32)
            step(total, 0, k, r)
            total = q_sum(k, mx, r)
            for j in xs:
                total += q2[j - 1, k, r].astype(f32)
            step(total, 1, k, r)

        rows(update)
        for j in ys:
            ay_copy(j, k, my).start()
        for j in xs:
            ax_copy(j, k, mx).start()
        d0_copy(k, core).start()

    each(third)

    def fourth(k):
        for jy in ys:
            ay_copy(jy, k, minus(my, jy, Y)).wait_recv()
            for jx in xs:
                rx_copy(jx, jy, k, mx).start()
            dy_copy(jy, k, core).start()
        for jx in xs:
            ax_copy(jx, k, minus(mx, jx, X)).wait_recv()
            for jy in ys:
                ry_copy(jx, jy, k, my).start()
            dx_copy(jx, k, core).start()

    each(fourth)

    def fifth(k):
        for jx in xs:
            for jy in ys:
                rx_copy(jx, jy, k, minus(mx, jx, X)).wait_recv()
                dp_copy(jx, jy, k, core).start()
                ry_copy(jx, jy, k, minus(my, jy, Y)).wait_recv()
                dq_copy(jx, jy, k, core).start()

    each(fifth)

    def finish(k):
        pair_copy(k).wait_send()
        d0_copy(k, other).wait()
        for jx in xs:
            p1_copy(jx, k).wait_send()
            q2_copy(jx, k).wait_send()
            ax_copy(jx, k, mx).wait_send()
            dx_copy(jx, k, other).wait()
            for jy in ys:
                rx_copy(jx, jy, k, mx).wait_send()
                ry_copy(jx, jy, k, my).wait_send()
                dp_copy(jx, jy, k, other).wait()
                dq_copy(jx, jy, k, other).wait()
        for jy in ys:
            q1_copy(jy, k).wait_send()
            p2_copy(jy, k).wait_send()
            ay_copy(jy, k, my).wait_send()
            dy_copy(jy, k, other).wait()

    each(finish)


def per_device(n, grad_parts, master, momentum):
    Y, X, C = factors(n)
    layers, rows, cols = master.shape
    tall = layers * rows
    half = tall // 2
    K = max(k for k in range(1, MOST_CHUNKS + 1) if half % (k * ROWS) == 0)
    c = half // K
    g = grad_parts.reshape(Y, X, C, 2, K, c, cols)
    state_shape = (2, K, c, cols)
    w_shape = (Y, X, C, 2, K, c, cols)
    scratch = [
        (K, Y, X, 2, c, cols), (K, Y, X, 2, c, cols),
        (X - 1, K, Y, c, cols), (Y - 1, K, X, c, cols),
        (Y - 1, K, c, cols), (X - 1, K, c, cols),
    ]
    sems = [(K,), (2, K)]
    for shape in ((K,), (X - 1, K), (Y - 1, K), (Y - 1, K), (X - 1, K),
                  (Y - 1, K), (X - 1, K), (X - 1, Y - 1, K), (X - 1, Y - 1, K),
                  (K,), (Y - 1, K), (X - 1, K), (X - 1, Y - 1, K), (X - 1, Y - 1, K)):
        sems += [shape, shape]
    size = lambda s: functools.reduce(lambda a, b: a * b, s)
    new_master, new_momentum, weights = pl.pallas_call(
        functools.partial(kernel, (Y, X, C, K, c)),
        out_shape=(
            pltpu.VMEM(state_shape, f32),
            pltpu.VMEM(state_shape, f32),
            pltpu.VMEM(w_shape, bf16),
        ),
        in_specs=[pl.BlockSpec(memory_space=pltpu.HBM)] * 3,
        out_specs=[pl.BlockSpec(memory_space=pltpu.VMEM)] * 3,
        scratch_shapes=[pltpu.VMEM(s, bf16) for s in scratch]
        + [pltpu.SemaphoreType.DMA(s) for s in sems],
        compiler_params=pltpu.CompilerParams(
            collective_id=0, has_side_effects=True,
            vmem_limit_bytes=sum(2 * size(s) for s in scratch) + (2 << 20),
        ),
    )(g, master.reshape(state_shape), momentum.reshape(state_shape))
    return (
        new_master.reshape(master.shape),
        new_momentum.reshape(master.shape),
        weights.reshape(layers, n * rows, cols),
    )


def solution(mesh):
    return jax.shard_map(
        functools.partial(per_device, mesh.shape["dp"]),
        mesh=mesh,
        in_specs=(P("dp", None, None, "mp"), P(None, "dp", "mp"), P(None, "dp", "mp")),
        out_specs=(P(None, "dp", "mp"), P(None, "dp", "mp"), P(None, None, "mp")),
        check_vma=False,
    )
```

```python
import functools

import jax
import jax.numpy as jnp
from jax import lax
from jax.experimental import pallas as pl
from jax.experimental.pallas import tpu as pltpu
from jax.sharding import PartitionSpec as P

beta_one = 0.9
beta_two = 0.99
step_size = 0.1
decay_rate = 0.1
softness = 0.05

f32 = jnp.float32
bf16 = jnp.bfloat16
MESH = pl.DeviceIdType.MESH
ROWS = 16
MOST_CHUNKS = 8


def factors(n):
    cores = 2
    across = 2
    return n // (cores * across), across, cores


def kernel(
    dims,
    g_ref, master_ref, momentum_ref,
    nmaster, nmomentum, w,
    own, pair, p1, q1, p2, q2,
    load_sem, state_sem,
    pair_s, pair_r, p1_s, p1_r, q1_s, q1_r, p2_s, p2_r, q2_s, q2_r,
    ay_s, ay_r, ax_s, ax_r, rx_s, rx_r, ry_s, ry_r,
    d0_s, d0_r, dy_s, dy_r, dx_s, dx_r, dp_s, dp_r, dq_s, dq_r,
):
    Y, X, C, K, c = dims
    me = lax.axis_index("dp")
    core = lax.rem(me, C)
    mx = lax.rem(me // C, X)
    my = me // (C * X)
    other = 1 - core

    def index(y, x, k):
        return {"dp": (y * X + x) * C + k}

    mate = index(my, mx, other)

    def plus(a, j, size):
        return lax.rem(a + j, size)

    def minus(a, j, size):
        return lax.rem(a + size - j, size)

    ys, xs = range(1, Y), range(1, X)

    def remote(src, dst, s, r, to):
        return pltpu.make_async_remote_copy(
            src_ref=src, dst_ref=dst, send_sem=s, recv_sem=r,
            device_id=to, device_id_type=MESH,
        )

    def load(k):
        return pltpu.make_async_copy(g_ref.at[:, :, core, :, k], own.at[k], load_sem.at[k])

    def state(k):
        return (
            pltpu.make_async_copy(master_ref.at[:, k], nmaster.at[:, k], state_sem.at[0, k]),
            pltpu.make_async_copy(momentum_ref.at[:, k], nmomentum.at[:, k], state_sem.at[1, k]),
        )

    def pair_copy(k):
        return remote(g_ref.at[:, :, other, :, k], pair.at[k], pair_s.at[k], pair_r.at[k], mate)

    def p1_copy(j, k):
        to = plus(mx, j, X)
        return remote(own.at[k, :, to, 0], p1.at[j - 1, k], p1_s.at[j - 1, k], p1_r.at[j - 1, k], index(my, to, core))

    def q1_copy(j, k):
        to = plus(my, j, Y)
        return remote(own.at[k, to, :, 1], q1.at[j - 1, k], q1_s.at[j - 1, k], q1_r.at[j - 1, k], index(to, mx, core))

    def p2_copy(j, k):
        to = plus(my, j, Y)
        return remote(own.at[k, to, mx, 0], p2.at[j - 1, k], p2_s.at[j - 1, k], p2_r.at[j - 1, k], index(to, mx, core))

    def q2_copy(j, k):
        to = plus(mx, j, X)
        return remote(own.at[k, my, to, 1], q2.at[j - 1, k], q2_s.at[j - 1, k], q2_r.at[j - 1, k], index(my, to, core))

    def spread(block, s, r, to):
        return remote(block, block, s, r, to)

    def ay_copy(j, k, y):
        return spread(w.at[y, mx, core, :, k], ay_s.at[j - 1, k], ay_r.at[j - 1, k], index(plus(my, j, Y), mx, core))

    def ax_copy(j, k, x):
        return spread(w.at[my, x, core, :, k], ax_s.at[j - 1, k], ax_r.at[j - 1, k], index(my, plus(mx, j, X), core))

    def rx_copy(jx, jy, k, x):
        y = minus(my, jy, Y)
        return spread(w.at[y, x, core, 0, k], rx_s.at[jx - 1, jy - 1, k], rx_r.at[jx - 1, jy - 1, k], index(my, plus(mx, jx, X), core))

    def ry_copy(jx, jy, k, y):
        x = minus(mx, jx, X)
        return spread(w.at[y, x, core, 1, k], ry_s.at[jx - 1, jy - 1, k], ry_r.at[jx - 1, jy - 1, k], index(plus(my, jy, Y), mx, core))

    def d0_copy(k, half):
        return spread(w.at[my, mx, half, :, k], d0_s.at[k], d0_r.at[k], mate)

    def dy_copy(j, k, half):
        return spread(w.at[minus(my, j, Y), mx, half, :, k], dy_s.at[j - 1, k], dy_r.at[j - 1, k], mate)

    def dx_copy(j, k, half):
        return spread(w.at[my, minus(mx, j, X), half, :, k], dx_s.at[j - 1, k], dx_r.at[j - 1, k], mate)

    def dp_copy(jx, jy, k, half):
        return spread(w.at[minus(my, jy, Y), minus(mx, jx, X), half, 0, k], dp_s.at[jx - 1, jy - 1, k], dp_r.at[jx - 1, jy - 1, k], mate)

    def dq_copy(jx, jy, k, half):
        return spread(w.at[minus(my, jy, Y), minus(mx, jx, X), half, 1, k], dq_s.at[jx - 1, jy - 1, k], dq_r.at[jx - 1, jy - 1, k], mate)

    def each(body):
        lax.fori_loop(0, K, lambda k, carry: (body(k), carry)[1], 0)

    def rows(body):
        lax.fori_loop(0, c // ROWS, lambda r, carry: (body(pl.ds(pl.multiple_of(r * ROWS, ROWS), ROWS)), carry)[1], 0)

    def start_loads(k):
        load(k).start()

    def start_state(k):
        for copy in state(k):
            copy.start()

    each(start_loads)

    barrier = pltpu.get_barrier_semaphore()
    peers = [mate]
    peers += [index(my, plus(mx, j, X), core) for j in xs]
    peers += [index(plus(my, j, Y), mx, core) for j in ys]
    for peer in peers:
        pl.semaphore_signal(barrier, inc=1, device_id=peer, device_id_type=MESH)
    pl.semaphore_wait(barrier, len(peers))

    each(lambda k: pair_copy(k).start())
    each(start_state)

    def first(k):
        load(k).wait()
        pair_copy(k).wait_recv()

        def add(r):
            for j in xs:
                x = plus(mx, j, X)
                for y in range(Y):
                    own[k, y, x, 0, r] = (own[k, y, x, 0, r].astype(f32) + pair[k, y, x, 0, r].astype(f32)).astype(bf16)
            for j in ys:
                y = plus(my, j, Y)
                for x in range(X):
                    own[k, y, x, 1, r] = (own[k, y, x, 1, r].astype(f32) + pair[k, y, x, 1, r].astype(f32)).astype(bf16)

        rows(add)
        for j in xs:
            p1_copy(j, k).start()
        for j in ys:
            q1_copy(j, k).start()

    each(first)

    def p_sum(k, y, r):
        total = own[k, y, mx, 0, r].astype(f32) + pair[k, y, mx, 0, r].astype(f32)
        for j in xs:
            total += p1[j - 1, k, y, r].astype(f32)
        return total

    def q_sum(k, x, r):
        total = own[k, my, x, 1, r].astype(f32) + pair[k, my, x, 1, r].astype(f32)
        for j in ys:
            total += q1[j - 1, k, x, r].astype(f32)
        return total

    def second(k):
        for j in xs:
            p1_copy(j, k).wait_recv()
        for j in ys:
            q1_copy(j, k).wait_recv()

        def add(r):
            for j in ys:
                y = plus(my, j, Y)
                own[k, y, mx, 0, r] = p_sum(k, y, r).astype(bf16)
            for j in xs:
                x = plus(mx, j, X)
                own[k, my, x, 1, r] = q_sum(k, x, r).astype(bf16)

        rows(add)
        for j in ys:
            p2_copy(j, k).start()
        for j in xs:
            q2_copy(j, k).start()

    each(second)

    def step(total, h, k, r):
        gradient = total * (1.0 / (Y * X * C))
        momentum = nmomentum[h, k, r]
        master = nmaster[h, k, r]
        interp = beta_one * momentum + (1.0 - beta_one) * gradient
        direction = interp * lax.rsqrt(interp * interp + softness * softness)
        new_master = master - step_size * (direction + decay_rate * master)
        nmaster[h, k, r] = new_master
        nmomentum[h, k, r] = beta_two * momentum + (1.0 - beta_two) * gradient
        w[my, mx, core, h, k, r] = new_master.astype(bf16)

    def third(k):
        for copy in state(k):
            copy.wait()
        for j in ys:
            p2_copy(j, k).wait_recv()
        for j in xs:
            q2_copy(j, k).wait_recv()

        def update(r):
            total = p_sum(k, my, r)
            for j in ys:
                total += p2[j - 1, k, r].astype(f32)
            step(total, 0, k, r)
            total = q_sum(k, mx, r)
            for j in xs:
                total += q2[j - 1, k, r].astype(f32)
            step(total, 1, k, r)

        rows(update)
        for j in ys:
            ay_copy(j, k, my).start()
        for j in xs:
            ax_copy(j, k, mx).start()
        d0_copy(k, core).start()

    each(third)

    def fourth(k):
        for jy in ys:
            ay_copy(jy, k, minus(my, jy, Y)).wait_recv()
            for jx in xs:
                rx_copy(jx, jy, k, mx).start()
            dy_copy(jy, k, core).start()
        for jx in xs:
            ax_copy(jx, k, minus(mx, jx, X)).wait_recv()
            for jy in ys:
                ry_copy(jx, jy, k, my).start()
            dx_copy(jx, k, core).start()

    each(fourth)

    def fifth(k):
        for jx in xs:
            for jy in ys:
                rx_copy(jx, jy, k, minus(mx, jx, X)).wait_recv()
                dp_copy(jx, jy, k, core).start()
                ry_copy(jx, jy, k, minus(my, jy, Y)).wait_recv()
                dq_copy(jx, jy, k, core).start()

    each(fifth)

    def finish(k):
        pair_copy(k).wait_send()
        d0_copy(k, other).wait()
        for jx in xs:
            p1_copy(jx, k).wait_send()
            q2_copy(jx, k).wait_send()
            ax_copy(jx, k, mx).wait_send()
            dx_copy(jx, k, other).wait()
            for jy in ys:
                rx_copy(jx, jy, k, mx).wait_send()
                ry_copy(jx, jy, k, my).wait_send()
                dp_copy(jx, jy, k, other).wait()
                dq_copy(jx, jy, k, other).wait()
        for jy in ys:
            q1_copy(jy, k).wait_send()
            p2_copy(jy, k).wait_send()
            ay_copy(jy, k, my).wait_send()
            dy_copy(jy, k, other).wait()

    each(finish)


def put_kernel(pieces, *refs):
    sources, targets, sem = refs[:3], refs[3:6], refs[6]
    copies = []
    for source, target, cut in zip(sources, targets, pieces):
        for at in cut:
            copies.append(pltpu.make_async_copy(source.at[at], target.at[at], sem.at[len(copies)]))
    for copy in copies:
        copy.start()
    for copy in copies:
        copy.wait()


def put(arrays):
    depths = (1, 1, 3)
    pieces = [[()] for _ in arrays]
    for i, depth in enumerate(depths):
        for d in range(depth):
            pieces[i] = [at + (k,) for at in pieces[i] for k in range(arrays[i].shape[d])]
    return pl.pallas_call(
        functools.partial(put_kernel, pieces),
        out_shape=[jax.ShapeDtypeStruct(a.shape, a.dtype) for a in arrays],
        in_specs=[pl.BlockSpec(memory_space=pltpu.VMEM)] * len(arrays),
        out_specs=[pl.BlockSpec(memory_space=pltpu.HBM)] * len(arrays),
        scratch_shapes=[pltpu.SemaphoreType.DMA((sum(len(cut) for cut in pieces),))],
        compiler_params=pltpu.CompilerParams(vmem_limit_bytes=1 << 20),
    )(*arrays)


def per_device(n, grad_parts, master, momentum):
    Y, X, C = factors(n)
    layers, rows, cols = master.shape
    tall = layers * rows
    half = tall // 2
    K = max(k for k in range(1, MOST_CHUNKS + 1) if half % (k * ROWS) == 0)
    c = half // K
    g = grad_parts.reshape(Y, X, C, 2, K, c, cols)
    state_shape = (2, K, c, cols)
    w_shape = (Y, X, C, 2, K, c, cols)
    scratch = [
        (K, Y, X, 2, c, cols), (K, Y, X, 2, c, cols),
        (X - 1, K, Y, c, cols), (Y - 1, K, X, c, cols),
        (Y - 1, K, c, cols), (X - 1, K, c, cols),
    ]
    sems = [(K,), (2, K)]
    for shape in ((K,), (X - 1, K), (Y - 1, K), (Y - 1, K), (X - 1, K),
                  (Y - 1, K), (X - 1, K), (X - 1, Y - 1, K), (X - 1, Y - 1, K),
                  (K,), (Y - 1, K), (X - 1, K), (X - 1, Y - 1, K), (X - 1, Y - 1, K)):
        sems += [shape, shape]
    size = lambda s: functools.reduce(lambda a, b: a * b, s)
    results = pl.pallas_call(
        functools.partial(kernel, (Y, X, C, K, c)),
        out_shape=(
            pltpu.VMEM(state_shape, f32),
            pltpu.VMEM(state_shape, f32),
            pltpu.VMEM(w_shape, bf16),
        ),
        in_specs=[pl.BlockSpec(memory_space=pltpu.HBM)] * 3,
        out_specs=[pl.BlockSpec(memory_space=pltpu.VMEM)] * 3,
        scratch_shapes=[pltpu.VMEM(s, bf16) for s in scratch]
        + [pltpu.SemaphoreType.DMA(s) for s in sems],
        compiler_params=pltpu.CompilerParams(
            collective_id=0, has_side_effects=True,
            vmem_limit_bytes=sum(2 * size(s) for s in scratch) + (2 << 20),
        ),
    )(g, master.reshape(state_shape), momentum.reshape(state_shape))
    new_master, new_momentum, weights = put(results)
    return (
        new_master.reshape(master.shape),
        new_momentum.reshape(master.shape),
        weights.reshape(layers, n * rows, cols),
    )


def solution(mesh):
    return jax.shard_map(
        functools.partial(per_device, mesh.shape["dp"]),
        mesh=mesh,
        in_specs=(P("dp", None, None, "mp"), P(None, "dp", "mp"), P(None, "dp", "mp")),
        out_specs=(P(None, "dp", "mp"), P(None, "dp", "mp"), P(None, None, "mp")),
        check_vma=False,
    )
```
